32 devices in a mesh: gx: 4 (over y, x), gy: 2 (over core), gz: 4 (over z).
Axes of the slice: x: 2, y: 2, z: 4, core: 2. Of those that a mesh axis runs over, the one named last changes fastest.
Arguments:
- measures: float32 [65536, 256], P(('gx', 'gy', 'gz')), may hold values from -6 to 6
- group_index: int32 [65536], P(('gx', 'gy', 'gz')), may hold values from 0 to 511, as said below
- distinct_keys: int32 [32, 512], P(('gx', 'gy', 'gz')), may hold values from 32 to 65567, as said below
- group_counts: int32 [32], P(('gx', 'gy', 'gz')), may hold values from 128 to 512, as said below
Outputs:
- group_sums: float32 [16384, 256], P(('gx', 'gy', 'gz'))
- group_rows: int32 [16384], P(('gx', 'gy', 'gz'))
- group_keys: int32 [16384], P(('gx', 'gy', 'gz'))
- group_total: int32 [], replicated
The draws below stay inside these ranges and needn't reach their ends.
Inputs may be any that keep to these rules, and one draw needn't show every extreme that they name: `group_counts`: every device has between 128 and 512 groups, and some device has exactly 512. `group_index`: each row's index lies below its device's group count, and every group of a device has at least one row. `distinct_keys`: each device's keys rise strictly; all keys of device d equal d modulo 32, so no key lives on two devices; entries at and past the device's count are unused.
All inputs are finite; a program needn't handle non-finite values.
Results may differ from the reference program's by a relative error of at most 0.0003.
Values sent between devices are 32-bit elements; how exact they have to be, the bound alone decides.
A program may use at most 64 MiB of HBM per device.

```python
import jax
import jax.numpy as jnp
from jax import lax

ROW_DEV = 2048
M = 256
GMAX = 512
ROWS = 65536
DEVICES = 32


def shared_counts(key):
    counts = jax.random.randint(jax.random.fold_in(key, 7), (DEVICES,), GMAX // 4, GMAX + 1)
    fullest = jax.random.randint(jax.random.fold_in(key, 8), (), 0, DEVICES)
    return counts.at[fullest].set(GMAX).astype(jnp.int32)


def draw_group_counts(key, part):
    return shared_counts(key)


def one_device(key, count):
    places = jnp.arange(ROW_DEV, dtype=jnp.int32)
    upper = jnp.minimum(jax.random.randint(jax.random.fold_in(key, 1), (ROW_DEV,), 1, GMAX + 1), count)
    picked = jax.random.randint(jax.random.fold_in(key, 2), (ROW_DEV,), 0, upper)
    picked = jnp.where(places < count, places, picked % count)
    order = jax.random.permutation(jax.random.fold_in(key, 3), ROW_DEV)
    return picked[order].astype(jnp.int32)


def draw_group_index(key, part):
    counts = shared_counts(key)
    device_keys = jax.vmap(lambda d: jax.random.fold_in(jax.random.fold_in(key, 11), d))(jnp.arange(DEVICES))
    return jax.vmap(one_device)(device_keys, counts).reshape(-1)


def draw_distinct_keys(key, part):
    steps = jax.random.randint(jax.random.fold_in(key, 21), (DEVICES, GMAX), 1, 5)
    steps = steps.at[0, 0].set(1)
    rising = jnp.cumsum(steps, axis=1)
    rising = rising.at[:, GMAX - 1].set(4 * GMAX)
    owner = jnp.arange(DEVICES, dtype=jnp.int32)[:, None]
    return (owner + DEVICES * rising).astype(jnp.int32)


def shard_levels(key, extent, pieces, least, top_value):
    loudness = 1.0
    for dim, blocks in pieces:
        draws = jax.random.uniform(jax.random.fold_in(jax.random.fold_in(key, 6), dim), (blocks,), jnp.float32, least / len(pieces), top_value / len(pieces))
        loudness = loudness * jnp.repeat(jnp.exp(draws), extent[dim] // blocks).reshape((-1,) + (1,) * (len(extent) - 1 - dim))
    return loudness


def gaussian(key, dims, width, limit, split=(), held_as=jnp.bfloat16):
    drawn = width * jax.random.normal(key, dims, jnp.float32)
    if split:
        drawn = drawn * shard_levels(key, dims, split, -0.22, 0.18)
    return jnp.clip(drawn, -limit, limit).astype(held_as)


def setup_inputs(seed: int = 0) -> dict:
    arg_keys = jax.random.split(jax.random.key(seed), 5)
    measures = gaussian(arg_keys[0], (ROWS, M), 1.0, 6.0, ((0, 32),), jnp.float32)
    group_index = draw_group_index(jax.random.fold_in(arg_keys[4], 71), 0)
    distinct_keys = draw_distinct_keys(jax.random.fold_in(arg_keys[4], 71), 0)
    group_counts = draw_group_counts(jax.random.fold_in(arg_keys[4], 71), 0)
    return dict(measures=measures, group_index=group_index, distinct_keys=distinct_keys, group_counts=group_counts)


def local_groups(pair):
    values, index = pair
    sums = jax.ops.segment_sum(values, index, num_segments=GMAX)
    rows = jax.ops.segment_sum(jnp.ones_like(index), index, num_segments=GMAX)
    return sums, rows


def reference(measures, group_index, distinct_keys, group_counts):
    offsets = jnp.cumsum(group_counts) - group_counts
    group_total = jnp.sum(group_counts).astype(jnp.int32)
    values = measures.reshape(DEVICES, ROW_DEV, M)
    index = group_index.reshape(DEVICES, ROW_DEV)
    sums, rows = lax.map(local_groups, (values, index))
    local = jnp.arange(GMAX, dtype=jnp.int32)
    dense = offsets[:, None] + local[None, :]
    live = local[None, :] < group_counts[:, None]
    where_to = (dense % DEVICES) * GMAX + dense // DEVICES
    where_to = jnp.where(live, where_to, DEVICES * GMAX).astype(jnp.int32).reshape(-1)
    group_sums = jnp.zeros((DEVICES * GMAX, M), jnp.float32).at[where_to].set(sums.reshape(-1, M), mode="drop")
    group_rows = jnp.zeros((DEVICES * GMAX,), jnp.int32).at[where_to].set(rows.reshape(-1).astype(jnp.int32), mode="drop")
    group_keys = jnp.full((DEVICES * GMAX,), -1, jnp.int32).at[where_to].set(distinct_keys.reshape(-1), mode="drop")
    return group_sums, group_rows, group_keys, group_total
```

```python
import functools

import jax
import jax.numpy as jnp
from jax import lax
from jax.experimental import pallas as pl
from jax.experimental.pallas import tpu as pltpu
from jax.sharding import PartitionSpec as P

AXES = ("gx", "gy", "gz")
LANES = 128
MESH = pl.DeviceIdType.MESH


def round_up(value, unit):
    return (value + unit - 1) // unit * unit


def exchange_kernel(
    shape,
    index_ref,
    keys_ref,
    count_ref,
    measures_ref,
    recv_ref,
    counts_ref,
    held,
    stage,
    send,
    tally_ref,
    cbuf,
    load_sem,
    csend_sem,
    crecv_sem,
    send_sem,
    recv_sem,
):
    devices, ny, nz, span, levels, chunks, fields_at = shape
    me = (lax.axis_index("gx") * ny + lax.axis_index("gy")) * nz + lax.axis_index("gz")
    rows, width = held.shape
    chunk = rows // chunks
    halves = width // LANES
    sent_rows = fields_at + 2

    loads = []
    for c in range(chunks):
        piece = pl.ds(c * chunk, chunk)
        load = pltpu.make_async_copy(measures_ref.at[piece], held.at[piece], load_sem.at[c])
        load.start()
        loads.append(load)

    def place(k):
        other = lax.rem(me + k, devices)
        return other, (other // (ny * nz), lax.rem(other // nz, ny), lax.rem(other, nz))

    barrier = pltpu.get_barrier_semaphore()

    def greet(k, carry):
        _, spot = place(k)
        pl.semaphore_signal(barrier, inc=1, device_id=spot, device_id_type=MESH)
        return carry

    lax.fori_loop(1, devices, greet, 0)
    cbuf[pl.ds(me, 1), :, :] = jnp.full((1,) + cbuf.shape[1:], count_ref[0], jnp.int32)

    def count_copy(k, slot):
        other, spot = place(k)
        mine = cbuf.at[pl.ds(me, 1)]
        return pltpu.make_async_remote_copy(
            src_ref=mine,
            dst_ref=cbuf.at[pl.ds(slot(other), 1)],
            send_sem=csend_sem.at[other],
            recv_sem=crecv_sem.at[slot(other)],
            device_id=spot,
            device_id_type=MESH,
        )

    def data_copy(k, slot):
        other, spot = place(k)
        return pltpu.make_async_remote_copy(
            src_ref=send.at[other, pl.ds(0, sent_rows)],
            dst_ref=recv_ref.at[slot(other), pl.ds(0, sent_rows)],
            send_sem=send_sem.at[other],
            recv_sem=recv_sem.at[slot(other)],
            device_id=spot,
            device_id_type=MESH,
        )

    def start_all(make):
        def body(k, carry):
            make(k, lambda other: me).start()
            return carry

        lax.fori_loop(1, devices, body, 0)

    def wait_recv_all(make):
        def body(k, carry):
            make(k, lambda other: other).wait_recv()
            return carry

        lax.fori_loop(1, devices, body, 0)

    def wait_send_all(make):
        def body(k, carry):
            make(k, lambda other: me).wait_send()
            return carry

        lax.fori_loop(1, devices, body, 0)

    row = lax.broadcasted_iota(jnp.int32, (span, LANES), 0)
    labels = lax.rem(row, levels) * devices + row // levels

    total = None
    for c in range(chunks):
        loads[c].wait()
        x = held[pl.ds(c * chunk, chunk), :]
        high = x.astype(jnp.bfloat16)
        low = (x - high.astype(jnp.float32)).astype(jnp.bfloat16)
        parts = []
        for j in range(chunk // LANES):
            at = c * (chunk // LANES) + j
            hit = jnp.where(index_ref[pl.ds(at, 1), :] == labels, 1.0, 0.0)
            if at == 0:
                tally_ref[...] = hit
            else:
                tally_ref[...] += hit
            parts.append(hit.astype(jnp.bfloat16))
        hits = jnp.concatenate(parts, axis=1)
        dot = functools.partial(jnp.dot, preferred_element_type=jnp.float32)
        part = dot(hits, high) + dot(hits, low)
        for h in range(halves):
            block = part[:, h * LANES : (h + 1) * LANES].reshape(devices, levels, LANES)
            if c == 0:
                stage[:, h * levels : (h + 1) * levels, :] = block
            else:
                stage[:, h * levels : (h + 1) * levels, :] += block
        if c == 0:
            pl.semaphore_wait(barrier, devices - 1)
            start_all(count_copy)

    tallies = lax.dot_general(
        jnp.ones((8, LANES), jnp.bfloat16),
        tally_ref[...].astype(jnp.bfloat16),
        (((1,), (1,)), ((), ())),
        preferred_element_type=jnp.float32,
    )[0:1]
    keys = keys_ref[...]
    source = lax.broadcasted_iota(jnp.int32, (span, span), 0)
    goal = lax.broadcasted_iota(jnp.int32, (span, span), 1)
    moved = (source == lax.rem(goal, levels) * devices + goal // levels)
    moved = jnp.where(moved, 1.0, 0.0).astype(jnp.bfloat16)
    line = lax.broadcasted_iota(jnp.int32, (8, span), 0)
    pieces = jnp.where(
        line == 0, keys & 255, jnp.where(line == 1, (keys >> 8) & 255, (keys >> 16) & 255)
    )
    pieces = jnp.dot(
        pieces.astype(jnp.float32).astype(jnp.bfloat16), moved, preferred_element_type=jnp.float32
    )
    placed = pieces[0:1] + pieces[1:2] * 256.0 + pieces[2:3] * 65536.0
    fields = jnp.concatenate([tallies, placed], axis=0)
    for a in range(devices):
        tile = a * levels // LANES * LANES
        stage[a, fields_at : fields_at + 2, :] = fields[:, tile : tile + LANES]

    wait_recv_all(count_copy)
    counts = cbuf[...][:, 0, :]
    sender = lax.broadcasted_iota(jnp.int32, counts.shape, 0)
    lane = lax.broadcasted_iota(jnp.int32, counts.shape, 1)
    counts_ref[...] = jnp.sum(jnp.where(sender == lane, counts, 0), axis=0, keepdims=True)
    before = jnp.sum(jnp.where(sender < me, counts, 0), axis=0, keepdims=True)[0, 0]
    shift = lax.rem(before, devices)

    def roll(k, carry):
        other = lax.rem(me + k, devices)
        send[other] = stage[lax.rem(other - shift + devices, devices)]
        return carry

    lax.fori_loop(1, devices, roll, 0)
    recv_ref[me] = stage[lax.rem(me - shift + devices, devices)]
    start_all(data_copy)
    wait_send_all(count_copy)
    wait_recv_all(data_copy)
    wait_send_all(data_copy)


def place_kernel(
    shape, counts_ref, recv_ref, sums_ref, rows_ref, keys_ref, total_ref, buf
):
    devices, ny, nz, span, levels, fields_at = shape
    me = (lax.axis_index("gx") * ny + lax.axis_index("gy")) * nz + lax.axis_index("gz")
    halves = sums_ref.shape[1] // LANES
    lane = lax.broadcasted_iota(jnp.int32, (8, span), 1)
    fields = jnp.zeros((8, span), jnp.float32)
    offset = jnp.int32(0)

    def step(d, carry):
        offset, fields = carry
        count = counts_ref[0, d]
        first = lax.rem(me - lax.rem(offset, devices) + devices, devices)
        start = (offset + first) // devices
        for h in range(halves):
            buf[h, pl.ds(start, levels), :] = recv_ref[d, h * levels : (h + 1) * levels, :]
        base = lax.rem(first * levels, LANES)
        turn = lax.rem(lax.rem(start, LANES) - base + LANES, LANES)
        tile = recv_ref[d, fields_at : fields_at + 8, :]
        turned = pltpu.roll(tile, turn, 1)
        wide = jnp.concatenate([turned] * (span // LANES), axis=1)
        fields = jnp.where(lane >= start, wide, fields)
        return offset + count, fields

    offset, fields = lax.fori_loop(0, devices, step, (offset, fields), unroll=4)
    total_ref[0, 0] = offset
    taken = (offset - me + devices - 1) // devices
    row = lax.broadcasted_iota(jnp.int32, (span, LANES), 0)
    for h in range(halves):
        sums_ref[:, h * LANES : (h + 1) * LANES] = jnp.where(row < taken, buf[h, 0:span, :], 0.0)
    inside = lane[0:1] < taken
    rows_ref[...] = jnp.where(inside, fields[0:1].astype(jnp.int32), 0)
    keys_ref[...] = jnp.where(inside, fields[1:2].astype(jnp.int32), -1)


def shards(measures, group_index, distinct_keys, group_counts):
    rows, width = measures.shape
    span = distinct_keys.shape[1]
    ny, nz = lax.axis_size("gy"), lax.axis_size("gz")
    devices = lax.axis_size("gx") * ny * nz
    levels = span // devices
    chunks = 4 if rows % (4 * LANES) == 0 else 1
    fields_at = round_up(levels * (width // LANES), 8)
    slab = fields_at + 8
    wide = round_up(devices, LANES)
    vmem = pl.BlockSpec(memory_space=pltpu.VMEM)
    smem = pl.BlockSpec(memory_space=pltpu.SMEM)
    anywhere = pl.BlockSpec(memory_space=pl.ANY)
    received, counts = pl.pallas_call(
        functools.partial(
            exchange_kernel, (devices, ny, nz, span, levels, chunks, fields_at)
        ),
        out_shape=(
            jax.ShapeDtypeStruct((devices, slab, LANES), jnp.float32),
            jax.ShapeDtypeStruct((1, wide), jnp.int32),
        ),
        in_specs=[vmem, vmem, smem, anywhere],
        out_specs=(vmem, vmem),
        scratch_shapes=[
            pltpu.VMEM((rows, width), jnp.float32),
            pltpu.VMEM((devices, slab, LANES), jnp.float32),
            pltpu.VMEM((devices, slab, LANES), jnp.float32),
            pltpu.VMEM((span, LANES), jnp.float32),
            pltpu.VMEM((devices, 1, wide), jnp.int32),
            pltpu.SemaphoreType.DMA((chunks,)),
            pltpu.SemaphoreType.DMA((devices,)),
            pltpu.SemaphoreType.DMA((devices,)),
            pltpu.SemaphoreType.DMA((devices,)),
            pltpu.SemaphoreType.DMA((devices,)),
        ],
        compiler_params=pltpu.CompilerParams(collective_id=0, has_side_effects=True),
        name="exchange",
    )(group_index.reshape(rows // LANES, LANES), distinct_keys, group_counts, measures)
    sums, tallies, keys, total = pl.pallas_call(
        functools.partial(place_kernel, (devices, ny, nz, span, levels, fields_at)),
        out_shape=(
            jax.ShapeDtypeStruct((span, width), jnp.float32),
            jax.ShapeDtypeStruct((1, span), jnp.int32),
            jax.ShapeDtypeStruct((1, span), jnp.int32),
            jax.ShapeDtypeStruct((1, 1), jnp.int32),
        ),
        in_specs=[smem, vmem],
        out_specs=(vmem, vmem, vmem, smem),
        scratch_shapes=[pltpu.VMEM((width // LANES, span + round_up(levels, 8), LANES), jnp.float32)],
        name="place",
    )(counts, received)
    return sums, tallies.reshape(span), keys.reshape(span), total.reshape(())


def solution(mesh):
    return jax.shard_map(
        shards,
        mesh=mesh,
        in_specs=(
            P(AXES, None),
            P(AXES),
            P(AXES, None),
            P(AXES),
        ),
        out_specs=(P(AXES, None), P(AXES), P(AXES), P()),
        check_vma=False,
    )
```

```python
import functools

import jax
import jax.numpy as jnp
from jax import lax
from jax.experimental import pallas as pl
from jax.experimental.pallas import tpu as pltpu
from jax.sharding import PartitionSpec as P

AXES = ("gx", "gy", "gz")
LANES = 128
MESH = pl.DeviceIdType.MESH


def round_up(value, unit):
    return (value + unit - 1) // unit * unit


def steps_of(dims):
    nx, ny, nz = dims
    far = [(a, b, c) for c in range(nz) for a in range(nx) for b in range(ny)]
    far.sort(key=lambda k: -min(k[2], nz - k[2]))
    return [((a * ny + b) * nz + c, (a, b, c)) for a, b, c in far if (a, b, c) != (0, 0, 0)]


def wrapped(value, size):
    return jnp.where(value >= size, value - size, value)


def modulo(value, size):
    if size & (size - 1) == 0:
        return value & (size - 1)
    return lax.rem(value, size)


def divide(value, size):
    if size & (size - 1) == 0:
        return lax.shift_right_arithmetic(value, jnp.int32(size.bit_length() - 1))
    return value // size


def exchange_kernel(
    shape,
    index_hbm,
    keys_hbm,
    count_hbm,
    measures_ref,
    recv_ref,
    counts_ref,
    held,
    stage,
    send,
    tally_ref,
    cbuf,
    index_ref,
    keys_ref,
    count_ref,
    small_sem,
    load_sem,
    count_sem,
    data_sem,
):
    dims, span, levels, chunks, fields_at = shape
    nx, ny, nz = dims
    devices = nx * ny * nz
    spots = [lax.axis_index(axis) for axis in AXES]
    me = (spots[0] * ny + spots[1]) * nz + spots[2]
    ring = [[wrapped(spot + k, size) for k in range(size)] for spot, size in zip(spots, dims)]
    rows, width = held.shape
    chunk = rows // chunks
    halves = width // LANES
    sent_rows = fields_at + 2
    steps = steps_of(dims)

    count_load = pltpu.make_async_copy(count_hbm, count_ref, small_sem.at[0])
    count_load.start()
    barrier = pltpu.get_barrier_semaphore()
    for _, k in steps:
        pl.semaphore_signal(
            barrier, inc=1, device_id=tuple(r[i] for r, i in zip(ring, k)), device_id_type=MESH
        )
    index_load = pltpu.make_async_copy(index_hbm, index_ref, small_sem.at[1])
    index_load.start()
    loads = []
    for c in range(chunks):
        piece = pl.ds(c * chunk, chunk)
        load = pltpu.make_async_copy(measures_ref.at[piece], held.at[piece], load_sem.at[c])
        load.start()
        loads.append(load)
    keys_load = pltpu.make_async_copy(keys_hbm, keys_ref, small_sem.at[2])
    keys_load.start()

    def remote(source, goal, sems, k):
        return pltpu.make_async_remote_copy(
            src_ref=source,
            dst_ref=goal,
            send_sem=sems.at[0],
            recv_sem=sems.at[1],
            device_id=tuple(r[i] for r, i in zip(ring, k)),
            device_id_type=MESH,
        )

    count_load.wait()
    cbuf[0] = jnp.broadcast_to(count_ref[...], cbuf.shape[1:])
    index_load.wait()

    row = lax.broadcasted_iota(jnp.int32, (span, LANES), 0)
    labels = lax.rem(row, levels) * devices + row // levels

    total = None
    for c in range(chunks):
        loads[c].wait()
        x = held[pl.ds(c * chunk, chunk), :]
        high = x.astype(jnp.bfloat16)
        low = (x - high.astype(jnp.float32)).astype(jnp.bfloat16)
        parts = []
        for j in range(chunk // LANES):
            at = c * (chunk // LANES) + j
            hit = jnp.where(index_ref[pl.ds(at, 1), :] == labels, 1.0, 0.0)
            if at == 0:
                tally_ref[...] = hit
            else:
                tally_ref[...] += hit
            parts.append(hit.astype(jnp.bfloat16))
        hits = jnp.concatenate(parts, axis=1)
        dot = functools.partial(jnp.dot, preferred_element_type=jnp.float32)
        part = dot(hits, high) + dot(hits, low)
        for h in range(halves):
            block = part[:, h * LANES : (h + 1) * LANES].reshape(devices, levels, LANES)
            if c == 0:
                stage[:, h * levels : (h + 1) * levels, :] = block
            else:
                stage[:, h * levels : (h + 1) * levels, :] += block
        if c == 0:
            pl.semaphore_wait(barrier, devices - 1)
            for slot, k in steps:
                remote(cbuf.at[0], cbuf.at[slot], count_sem, k).start()

    tallies = lax.dot_general(
        jnp.ones((8, LANES), jnp.bfloat16),
        tally_ref[...].astype(jnp.bfloat16),
        (((1,), (1,)), ((), ())),
        preferred_element_type=jnp.float32,
    )[0:1]
    keys_load.wait()
    keys = keys_ref[...]
    source = lax.broadcasted_iota(jnp.int32, (span, span), 0)
    goal = lax.broadcasted_iota(jnp.int32, (span, span), 1)
    moved = (source == lax.rem(goal, levels) * devices + goal // levels)
    moved = jnp.where(moved, 1.0, 0.0).astype(jnp.bfloat16)
    line = lax.broadcasted_iota(jnp.int32, (8, span), 0)
    pieces = jnp.where(
        line == 0, keys & 255, jnp.where(line == 1, (keys >> 8) & 255, (keys >> 16) & 255)
    )
    pieces = jnp.dot(
        pieces.astype(jnp.float32).astype(jnp.bfloat16), moved, preferred_element_type=jnp.float32
    )
    placed = pieces[0:1] + pieces[1:2] * 256.0 + pieces[2:3] * 65536.0
    fields = jnp.concatenate([tallies, placed], axis=0)
    for a in range(devices):
        tile = a * levels // LANES * LANES
        stage[a, fields_at : fields_at + 2, :] = fields[:, tile : tile + LANES]

    others = cbuf.at[pl.ds(1, devices - 1)]
    pltpu.make_async_copy(others, others, count_sem.at[1]).wait()
    counts = cbuf[...][:, 0, :]
    slots = lax.broadcasted_iota(jnp.int32, counts.shape, 0)
    parts = (divide(slots, ny * nz), modulo(divide(slots, nz), ny), modulo(slots, nz))
    back = [
        jnp.where(spot >= part, spot - part, spot - part + size)
        for spot, part, size in zip(spots, parts, dims)
    ]
    sender = (back[0] * ny + back[1]) * nz + back[2]
    lane = lax.broadcasted_iota(jnp.int32, counts.shape, 1)
    counts_ref[...] = jnp.sum(jnp.where(sender == lane, counts, 0), axis=0, keepdims=True)
    before = jnp.sum(jnp.where(sender < me, counts, 0), axis=0, keepdims=True)[0, 0]
    shift = modulo(before, devices)

    for slot, (a, b, c) in steps:
        other = (ring[0][a] * ny + ring[1][b]) * nz + ring[2][c]
        send[slot] = stage[modulo(other - shift + devices, devices)]
    for slot, k in steps:
        piece = pl.ds(0, sent_rows)
        remote(send.at[slot, piece], recv_ref.at[slot, piece], data_sem, k).start()
    recv_ref[0] = stage[modulo(me - shift + devices, devices)]
    pltpu.make_async_copy(others, others, count_sem.at[0]).wait()
    landed = recv_ref.at[pl.ds(1, devices - 1), pl.ds(0, sent_rows)]
    left = send.at[pl.ds(1, devices - 1), pl.ds(0, sent_rows)]
    pltpu.make_async_copy(left, left, data_sem.at[0]).wait()
    pltpu.make_async_copy(landed, landed, data_sem.at[1]).wait()


def place_kernel(
    shape, counts_ref, recv_ref, sums_ref, rows_ref, keys_ref, total_ref, buf
):
    dims, span, levels, fields_at = shape
    nx, ny, nz = dims
    devices = nx * ny * nz
    spots = [lax.axis_index(axis) for axis in AXES]
    me = (spots[0] * ny + spots[1]) * nz + spots[2]
    back = [
        [jnp.where(spot >= k, spot - k, spot - k + size) for k in range(size)]
        for spot, size in zip(spots, dims)
    ]
    halves = sums_ref.shape[1] // LANES
    lane = lax.broadcasted_iota(jnp.int32, (8, span), 1)
    fields = jnp.zeros((8, span), jnp.float32)
    offset = jnp.int32(0)

    for d in range(devices):
        slot = (back[0][d // (ny * nz)] * ny + back[1][d // nz % ny]) * nz + back[2][d % nz]
        first = modulo(me - modulo(offset, devices) + devices, devices)
        start = divide(offset + first, devices)
        for h in range(halves):
            buf[h, pl.ds(start, levels), :] = recv_ref[slot, h * levels : (h + 1) * levels, :]
        turn = modulo(modulo(start, LANES) - modulo(first * levels, LANES) + LANES, LANES)
        turned = pltpu.roll(recv_ref[slot, fields_at : fields_at + 8, :], turn, 1)
        wide = jnp.concatenate([turned] * (span // LANES), axis=1)
        fields = jnp.where(lane >= start, wide, fields)
        offset = offset + counts_ref[0, d]

    total_ref[0, 0] = offset
    taken = divide(offset - me + devices - 1, devices)
    row = lax.broadcasted_iota(jnp.int32, (span, LANES), 0)
    for h in range(halves):
        sums_ref[:, h * LANES : (h + 1) * LANES] = jnp.where(row < taken, buf[h, 0:span, :], 0.0)
    inside = lane[0:1] < taken
    rows_ref[...] = jnp.where(inside, fields[0:1].astype(jnp.int32), 0)
    keys_ref[...] = jnp.where(inside, fields[1:2].astype(jnp.int32), -1)


def shards(measures, group_index, distinct_keys, group_counts):
    rows, width = measures.shape
    span = distinct_keys.shape[1]
    dims = tuple(lax.axis_size(axis) for axis in AXES)
    devices = dims[0] * dims[1] * dims[2]
    levels = span // devices
    chunks = 4 if rows % (4 * LANES) == 0 else 1
    fields_at = round_up(levels * (width // LANES), 8)
    slab = fields_at + 8
    wide = round_up(devices, LANES)
    vmem = pl.BlockSpec(memory_space=pltpu.VMEM)
    smem = pl.BlockSpec(memory_space=pltpu.SMEM)
    anywhere = pl.BlockSpec(memory_space=pl.ANY)
    received, counts = pl.pallas_call(
        functools.partial(
            exchange_kernel, (dims, span, levels, chunks, fields_at)
        ),
        out_shape=(
            jax.ShapeDtypeStruct((devices, slab, LANES), jnp.float32),
            jax.ShapeDtypeStruct((1, wide), jnp.int32),
        ),
        in_specs=[anywhere] * 4,
        out_specs=(vmem, vmem),
        scratch_shapes=[
            pltpu.VMEM((rows, width), jnp.float32),
            pltpu.VMEM((devices, slab, LANES), jnp.float32),
            pltpu.VMEM((devices, slab, LANES), jnp.float32),
            pltpu.VMEM((span, LANES), jnp.float32),
            pltpu.VMEM((devices, 1, wide), jnp.int32),
            pltpu.VMEM((rows // LANES, LANES), jnp.int32),
            pltpu.VMEM((1, span), jnp.int32),
            pltpu.VMEM((1, 1), jnp.int32),
            pltpu.SemaphoreType.DMA((3,)),
            pltpu.SemaphoreType.DMA((chunks,)),
            pltpu.SemaphoreType.DMA((2,)),
            pltpu.SemaphoreType.DMA((2,)),
        ],
        compiler_params=pltpu.CompilerParams(collective_id=0, has_side_effects=True),
        name="exchange",
    )(group_index.reshape(rows // LANES, LANES), distinct_keys, group_counts.reshape(1, 1), measures)
    sums, tallies, keys, total = pl.pallas_call(
        functools.partial(place_kernel, (dims, span, levels, fields_at)),
        out_shape=(
            jax.ShapeDtypeStruct((span, width), jnp.float32),
            jax.ShapeDtypeStruct((1, span), jnp.int32),
            jax.ShapeDtypeStruct((1, span), jnp.int32),
            jax.ShapeDtypeStruct((1, 1), jnp.int32),
        ),
        in_specs=[smem, vmem],
        out_specs=(vmem, vmem, vmem, smem),
        scratch_shapes=[pltpu.VMEM((width // LANES, span + round_up(levels, 8), LANES), jnp.float32)],
        name="place",
    )(counts, received)
    return sums, tallies.reshape(span), keys.reshape(span), total.reshape(())


def solution(mesh):
    return jax.shard_map(
        shards,
        mesh=mesh,
        in_specs=(
            P(AXES, None),
            P(AXES),
            P(AXES, None),
            P(AXES),
        ),
        out_specs=(P(AXES, None), P(AXES), P(AXES), P()),
        check_vma=False,
    )
```

```python
import functools

import jax
import jax.numpy as jnp
from jax import lax
from jax.experimental import pallas as pl
from jax.experimental.pallas import tpu as pltpu
from jax.sharding import PartitionSpec as P

AXES = ("gx", "gy", "gz")
LANES = 128
MESH = pl.DeviceIdType.MESH


def round_up(value, unit):
    return (value + unit - 1) // unit * unit


def steps_of(dims):
    nx, ny, nz = dims
    far = [(a, b, c) for c in range(nz) for a in range(nx) for b in range(ny)]
    far.sort(key=lambda k: -min(k[2], nz - k[2]))
    return [((a * ny + b) * nz + c, (a, b, c)) for a, b, c in far if (a, b, c) != (0, 0, 0)]


def wrapped(value, size):
    return jnp.where(value >= size, value - size, value)


def modulo(value, size):
    if size & (size - 1) == 0:
        return value & (size - 1)
    return lax.rem(value, size)


def divide(value, size):
    if size & (size - 1) == 0:
        return lax.shift_right_arithmetic(value, jnp.int32(size.bit_length() - 1))
    return value // size


def exchange_kernel(
    shape,
    index_hbm,
    keys_hbm,
    count_hbm,
    measures_ref,
    recv_ref,
    counts_ref,
    held,
    stage,
    send,
    tally_ref,
    cbuf,
    index_ref,
    keys_ref,
    count_ref,
    small_sem,
    load_sem,
    count_sem,
    data_sem,
):
    dims, span, levels, chunks, fields_at = shape
    nx, ny, nz = dims
    devices = nx * ny * nz
    spots = [lax.axis_index(axis) for axis in AXES]
    me = (spots[0] * ny + spots[1]) * nz + spots[2]
    ring = [[wrapped(spot + k, size) for k in range(size)] for spot, size in zip(spots, dims)]
    rows, width = held.shape
    chunk = rows // chunks
    halves = width // LANES
    sent_rows = fields_at + 2
    steps = steps_of(dims)

    count_load = pltpu.make_async_copy(count_hbm, count_ref, small_sem.at[0])
    count_load.start()
    barrier = pltpu.get_barrier_semaphore()
    for _, k in steps:
        pl.semaphore_signal(
            barrier, inc=1, device_id=tuple(r[i] for r, i in zip(ring, k)), device_id_type=MESH
        )
    index_load = pltpu.make_async_copy(index_hbm, index_ref, small_sem.at[1])
    index_load.start()
    loads = []
    for c in range(chunks):
        piece = pl.ds(c * chunk, chunk)
        load = pltpu.make_async_copy(measures_ref.at[piece], held.at[piece], load_sem.at[c])
        load.start()
        loads.append(load)
    keys_load = pltpu.make_async_copy(keys_hbm, keys_ref, small_sem.at[2])
    keys_load.start()

    def remote(source, goal, sems, k):
        return pltpu.make_async_remote_copy(
            src_ref=source,
            dst_ref=goal,
            send_sem=sems.at[0],
            recv_sem=sems.at[1],
            device_id=tuple(r[i] for r, i in zip(ring, k)),
            device_id_type=MESH,
        )

    count_load.wait()
    cbuf[0] = jnp.broadcast_to(count_ref[...], cbuf.shape[1:])
    index_load.wait()

    row = lax.broadcasted_iota(jnp.int32, (span, LANES), 0)
    labels = lax.rem(row, levels) * devices + row // levels

    total = None
    for c in range(chunks):
        loads[c].wait()
        x = held[pl.ds(c * chunk, chunk), :]
        high = x.astype(jnp.bfloat16)
        low = (x - high.astype(jnp.float32)).astype(jnp.bfloat16)
        parts = []
        for j in range(chunk // LANES):
            at = c * (chunk // LANES) + j
            hit = jnp.where(index_ref[pl.ds(at, 1), :] == labels, 1.0, 0.0)
            if at == 0:
                tally_ref[...] = hit
            else:
                tally_ref[...] += hit
            parts.append(hit.astype(jnp.bfloat16))
        hits = jnp.concatenate(parts, axis=1)
        dot = functools.partial(jnp.dot, preferred_element_type=jnp.float32)
        part = dot(hits, high) + dot(hits, low)
        for h in range(halves):
            block = part[:, h * LANES : (h + 1) * LANES].reshape(devices, levels, LANES)
            if c == 0:
                stage[:, h * levels : (h + 1) * levels, :] = block
            else:
                stage[:, h * levels : (h + 1) * levels, :] += block
        if c == 0:
            pl.semaphore_wait(barrier, devices - 1)
            for slot, k in steps:
                remote(cbuf.at[0], cbuf.at[slot], count_sem, k).start()

    tallies = lax.dot_general(
        jnp.ones((8, LANES), jnp.bfloat16),
        tally_ref[...].astype(jnp.bfloat16),
        (((1,), (1,)), ((), ())),
        preferred_element_type=jnp.float32,
    )[0:1]
    keys_load.wait()
    keys = keys_ref[...]
    source = lax.broadcasted_iota(jnp.int32, (span, span), 0)
    goal = lax.broadcasted_iota(jnp.int32, (span, span), 1)
    moved = (source == lax.rem(goal, levels) * devices + goal // levels)
    moved = jnp.where(moved, 1.0, 0.0).astype(jnp.bfloat16)
    line = lax.broadcasted_iota(jnp.int32, (8, span), 0)
    pieces = jnp.where(
        line == 0, keys & 255, jnp.where(line == 1, (keys >> 8) & 255, (keys >> 16) & 255)
    )
    pieces = jnp.dot(
        pieces.astype(jnp.float32).astype(jnp.bfloat16), moved, preferred_element_type=jnp.float32
    )
    placed = pieces[0:1] + pieces[1:2] * 256.0 + pieces[2:3] * 65536.0
    fields = jnp.concatenate([tallies, placed], axis=0)
    for a in range(devices):
        tile = a * levels // LANES * LANES
        stage[a, fields_at : fields_at + 2, :] = fields[:, tile : tile + LANES]

    others = cbuf.at[pl.ds(1, devices - 1)]
    pltpu.make_async_copy(others, others, count_sem.at[1]).wait()
    counts = cbuf[...][:, 0, :]
    slots = lax.broadcasted_iota(jnp.int32, counts.shape, 0)
    parts = (divide(slots, ny * nz), modulo(divide(slots, nz), ny), modulo(slots, nz))
    back = [
        jnp.where(spot >= part, spot - part, spot - part + size)
        for spot, part, size in zip(spots, parts, dims)
    ]
    sender = (back[0] * ny + back[1]) * nz + back[2]
    lane = lax.broadcasted_iota(jnp.int32, counts.shape, 1)
    counts_ref[...] = jnp.sum(jnp.where(sender == lane, counts, 0), axis=0, keepdims=True)
    before = jnp.sum(jnp.where(sender < me, counts, 0), axis=0, keepdims=True)[0, 0]
    shift = modulo(before, devices)

    for slot, (a, b, c) in steps:
        other = (ring[0][a] * ny + ring[1][b]) * nz + ring[2][c]
        send[slot] = stage[modulo(other - shift + devices, devices)]
    for slot, k in steps:
        piece = pl.ds(0, sent_rows)
        remote(send.at[slot, piece], recv_ref.at[slot, piece], data_sem, k).start()
    recv_ref[0] = stage[modulo(me - shift + devices, devices)]
    pltpu.make_async_copy(others, others, count_sem.at[0]).wait()
    landed = recv_ref.at[pl.ds(1, devices - 1), pl.ds(0, sent_rows)]
    left = send.at[pl.ds(1, devices - 1), pl.ds(0, sent_rows)]
    pltpu.make_async_copy(left, left, data_sem.at[0]).wait()
    pltpu.make_async_copy(landed, landed, data_sem.at[1]).wait()


def place_kernel(
    shape, counts_ref, recv_ref, sums_ref, rows_ref, keys_ref, total_ref, buf
):
    dims, span, levels, fields_at = shape
    nx, ny, nz = dims
    devices = nx * ny * nz
    spots = [lax.axis_index(axis) for axis in AXES]
    me = (spots[0] * ny + spots[1]) * nz + spots[2]
    back = [
        [jnp.where(spot >= k, spot - k, spot - k + size) for k in range(size)]
        for spot, size in zip(spots, dims)
    ]
    halves = sums_ref.shape[1] // LANES
    lane = lax.broadcasted_iota(jnp.int32, (8, span), 1)
    fields = jnp.zeros((8, span), jnp.float32)
    offset = jnp.int32(0)

    for d in range(devices):
        slot = (back[0][d // (ny * nz)] * ny + back[1][d // nz % ny]) * nz + back[2][d % nz]
        first = modulo(me - modulo(offset, devices) + devices, devices)
        start = divide(offset + first, devices)
        for h in range(halves):
            buf[h, pl.ds(start, levels), :] = recv_ref[slot, h * levels : (h + 1) * levels, :]
        turn = modulo(modulo(start, LANES) - modulo(first * levels, LANES) + LANES, LANES)
        turned = pltpu.roll(recv_ref[slot, fields_at : fields_at + 8, :], turn, 1)
        wide = jnp.concatenate([turned] * (span // LANES), axis=1)
        fields = jnp.where(lane >= start, wide, fields)
        offset = offset + counts_ref[0, d]

    total_ref[0, 0] = offset
    taken = divide(offset - me + devices - 1, devices)
    row = lax.broadcasted_iota(jnp.int32, (span, LANES), 0)
    for h in range(halves):
        sums_ref[:, h * LANES : (h + 1) * LANES] = jnp.where(row < taken, buf[h, 0:span, :], 0.0)
    inside = lane[0:1] < taken
    rows_ref[...] = jnp.where(inside, fields[0:1].astype(jnp.int32), 0)
    keys_ref[...] = jnp.where(inside, fields[1:2].astype(jnp.int32), -1)


def shards(measures, group_index, distinct_keys, group_counts):
    rows, width = measures.shape
    span = distinct_keys.shape[1]
    dims = tuple(lax.axis_size(axis) for axis in AXES)
    devices = dims[0] * dims[1] * dims[2]
    levels = span // devices
    chunks = 4 if rows % (4 * LANES) == 0 else 1
    fields_at = round_up(levels * (width // LANES), 8)
    slab = fields_at + 8
    wide = round_up(devices, LANES)
    vmem = pl.BlockSpec(memory_space=pltpu.VMEM)
    smem = pl.BlockSpec(memory_space=pltpu.SMEM)
    anywhere = pl.BlockSpec(memory_space=pl.ANY)
    received, counts = pl.pallas_call(
        functools.partial(
            exchange_kernel, (dims, span, levels, chunks, fields_at)
        ),
        out_shape=(
            pltpu.VMEM((devices, slab, LANES), jnp.float32),
            pltpu.VMEM((1, wide), jnp.int32),
        ),
        in_specs=[anywhere] * 4,
        out_specs=(vmem, vmem),
        scratch_shapes=[
            pltpu.VMEM((rows, width), jnp.float32),
            pltpu.VMEM((devices, slab, LANES), jnp.float32),
            pltpu.VMEM((devices, slab, LANES), jnp.float32),
            pltpu.VMEM((span, LANES), jnp.float32),
            pltpu.VMEM((devices, 1, wide), jnp.int32),
            pltpu.VMEM((rows // LANES, LANES), jnp.int32),
            pltpu.VMEM((1, span), jnp.int32),
            pltpu.VMEM((1, 1), jnp.int32),
            pltpu.SemaphoreType.DMA((3,)),
            pltpu.SemaphoreType.DMA((chunks,)),
            pltpu.SemaphoreType.DMA((2,)),
            pltpu.SemaphoreType.DMA((2,)),
        ],
        compiler_params=pltpu.CompilerParams(collective_id=0, has_side_effects=True),
        name="exchange",
    )(group_index.reshape(rows // LANES, LANES), distinct_keys, group_counts.reshape(1, 1), measures)
    sums, tallies, keys, total = pl.pallas_call(
        functools.partial(place_kernel, (dims, span, levels, fields_at)),
        out_shape=(
            jax.ShapeDtypeStruct((span, width), jnp.float32),
            jax.ShapeDtypeStruct((1, span), jnp.int32),
            jax.ShapeDtypeStruct((1, span), jnp.int32),
            jax.ShapeDtypeStruct((1, 1), jnp.int32),
        ),
        in_specs=[smem, vmem],
        out_specs=(vmem, vmem, vmem, smem),
        scratch_shapes=[pltpu.VMEM((width // LANES, span + round_up(levels, 8), LANES), jnp.float32)],
        compiler_params=pltpu.CompilerParams(vmem_limit_bytes=16 * 1024 * 1024),
        name="place",
    )(*(pltpu.with_memory_space_constraint(part, pltpu.VMEM) for part in (counts, received)))
    return sums, tallies.reshape(span), keys.reshape(span), total.reshape(())


def solution(mesh):
    return jax.shard_map(
        shards,
        mesh=mesh,
        in_specs=(
            P(AXES, None),
            P(AXES),
            P(AXES, None),
            P(AXES),
        ),
        out_specs=(P(AXES, None), P(AXES), P(AXES), P()),
        check_vma=False,
    )
```
